32 devices in a mesh: section: 2 (over x), dp: 16 (over z, y, core).
Axes of the slice: x: 2, y: 2, z: 4, core: 2. Of those that a mesh axis runs over, the one named last changes fastest.
Arguments:
- inputs: bfloat16 [2048, 8192], P('dp', 'section'), may hold values from -6 to 6
- cotangent: bfloat16 [2048, 8192], P('dp', 'section'), may hold values from -6 to 6
- weights: bfloat16 [2, 64, 8192], P('section'), may hold values from -0.0625 to 0.0625
- momentum: bfloat16 [2, 16, 64, 8192], P('section', 'dp'), may hold values from -6 to 6
- keep_index: int32 [2, 16, 128, 32], P('section', 'dp'), may hold values from 0 to 4095, as said below
Outputs:
- momentum_out: bfloat16 [2, 16, 64, 8192], P('section', 'dp')
- update: bfloat16 [2, 16, 64, 8192], P('section', 'dp')
The draws below stay inside these ranges and needn't reach their ends.
Inputs may be any that keep to these rules, and one draw needn't show every extreme that they name: `keep_index`: the 32 positions of one block of one replica and layer are all different.
All inputs are finite; a program needn't handle non-finite values.
Results may differ from the reference program's by a relative error of at most 0.0095.
Values may be sent and summed in bfloat16 or wider, within the bound.
A program may use at most 64 MiB of HBM per device.

```python
import math
import jax
import jax.numpy as jnp
from jax import lax

D = 8192
COLS = 64
K = 32
LAYERS = 2
REPLICAS = 16
TOKENS = 2048
GROUPS = 128


def draw_keep_index(key, part):
    sub_keys = jax.random.split(key, LAYERS * REPLICAS)

    def draw_rows(sub_key):
        scores = jax.random.randint(sub_key, (GROUPS, 4096), 0, 2 ** 18, dtype=jnp.int32)
        scores = scores * 4096 + jnp.arange(4096, dtype=jnp.int32)[None, :]
        return lax.top_k(scores, K)[1].astype(jnp.int32)
    return lax.map(draw_rows, sub_keys).reshape(LAYERS, REPLICAS, GROUPS, K)


def steps_of(rng, shape, cuts, low, top_value):
    factor_of = 1.0
    for dim, blocks in cuts:
        draws = jax.random.uniform(jax.random.fold_in(jax.random.fold_in(rng, 6), dim), (blocks,), jnp.float32, low / len(cuts), top_value / len(cuts))
        factor_of = factor_of * jnp.repeat(jnp.exp(draws), shape[dim] // blocks).reshape((-1,) + (1,) * (len(shape) - 1 - dim))
    return factor_of


def bell_draw(rng, dims, deviation, reach, shards=(), held_as=jnp.bfloat16):
    values = deviation * jax.random.normal(rng, dims, jnp.float32)
    if shards:
        values = values * steps_of(rng, dims, shards, -0.22, 0.18)
    return jnp.clip(values, -reach, reach).astype(held_as)


def setup_inputs(seed: int = 0) -> dict:
    key_of = jax.random.split(jax.random.key(seed), 6)
    inputs = bell_draw(key_of[0], (TOKENS, D), 1.0, 6.0, ((0, 16), (1, 2)))
    cotangent = bell_draw(key_of[1], (TOKENS, D), 1.0, 6.0, ((0, 16), (1, 2)))
    weights = bell_draw(key_of[2], (LAYERS, COLS, D), D ** -0.5, 0.0625, ((0, 2),))
    momentum = bell_draw(key_of[3], (LAYERS, REPLICAS, COLS, D), 1.0, 6.0, ((0, 2), (1, 16)))
    keep_index = draw_keep_index(jax.random.fold_in(key_of[5], 71), 0)
    return {"inputs": inputs, "cotangent": cotangent, "weights": weights, "momentum": momentum, "keep_index": keep_index}


DECAY = 0.999

def dct_basis(length):
    freq = jnp.arange(length, dtype=jnp.float32)[:, None]
    position = jnp.arange(length, dtype=jnp.float32)[None, :]
    dct_table = jnp.cos(math.pi * (position + 0.5) * freq / length) * math.sqrt(2.0 / length)
    return jnp.where(freq == 0, dct_table * math.sqrt(0.5), dct_table)

def forward_groups(field_in, dct_table):
    row_count, columns = field_in.shape[-2:]
    blocks = field_in.reshape(field_in.shape[:-2] + (row_count // 64, 64, columns // 64, 64))
    coeffs = jnp.einsum('kn,...anbm,jm->...akbj', dct_table, blocks, dct_table, precision=lax.Precision.HIGHEST)
    return coeffs.reshape(field_in.shape[:-2] + (-1,))

def inverse_groups(flat_in, dct_table, row_count, columns):
    blocks = flat_in.reshape(flat_in.shape[:-1] + (row_count // 64, 64, columns // 64, 64))
    field_out = jnp.einsum('kn,...akbj,jm->...anbm', dct_table, blocks, dct_table, precision=lax.Precision.HIGHEST)
    return field_out.reshape(flat_in.shape[:-1] + (row_count, columns))

def group_offsets(position, col_groups):
    group_id = jnp.arange(position.shape[-2], dtype=jnp.int32)[:, None]
    return group_id // col_groups * (4096 * col_groups) + position // 64 * (64 * col_groups) + group_id % col_groups * 64 + position % 64

def silu_slope(pre_act):
    sigma_h = jax.nn.sigmoid(pre_act)
    return sigma_h * (1.0 + pre_act * (1.0 - sigma_h))

def reference(inputs, cotangent, weights, momentum, keep_index):
    layers = weights.shape[0]
    replicas = momentum.shape[1]
    row_count, columns = (weights.shape[1], weights.shape[2])
    dct_table = dct_basis(64)
    activation = inputs
    saved_acts = []
    for layer_idx in range(layers):
        weight = weights[layer_idx]
        pre_act = jnp.dot(activation, weight.T, preferred_element_type=jnp.float32)
        gated_act = jax.nn.silu(pre_act).astype(jnp.bfloat16)
        saved_acts.append((activation, gated_act, pre_act))
        activation = (activation.astype(jnp.float32) + jnp.dot(gated_act, weight, preferred_element_type=jnp.float32)).astype(jnp.bfloat16)

    def by_replica(value):
        return value.astype(jnp.float32).reshape(replicas, -1, value.shape[-1])
    grad_in = cotangent
    moment_list = [None] * layers
    update_list = [None] * layers
    for layer_idx in reversed(range(layers)):
        activation, gated_act, pre_act = saved_acts[layer_idx]
        weight = weights[layer_idx]
        errors = jnp.dot(grad_in, weight.T, preferred_element_type=jnp.float32)
        deltas = (errors * silu_slope(pre_act)).astype(jnp.bfloat16)
        grad_total = jnp.einsum('rtc,rtd->rcd', by_replica(gated_act), by_replica(grad_in), precision=lax.Precision.HIGHEST)
        grad_total = grad_total + jnp.einsum('rtc,rtd->rcd', by_replica(deltas), by_replica(activation), precision=lax.Precision.HIGHEST)
        grad_in = (grad_in.astype(jnp.float32) + jnp.dot(deltas, weight, preferred_element_type=jnp.float32)).astype(jnp.bfloat16)
        momentum_new = DECAY * momentum[layer_idx].astype(jnp.float32) + grad_total
        coeffs = forward_groups(momentum_new, dct_table)
        offsets = group_offsets(keep_index[layer_idx], columns // 64).reshape(replicas, -1)
        kept_values = jnp.take_along_axis(coeffs, offsets, axis=1)
        replica_ids = jnp.arange(replicas, dtype=jnp.int32)[:, None] + jnp.zeros_like(offsets)
        sparse = jnp.zeros_like(coeffs).at[replica_ids, offsets].add(kept_values)
        own_field = inverse_groups(sparse, dct_table, row_count, columns)
        moment_list[layer_idx] = (momentum_new - own_field).astype(jnp.bfloat16)
        summed = lax.optimization_barrier(jnp.sum(sparse, axis=0))
        combined = inverse_groups(summed, dct_table, row_count, columns).astype(jnp.bfloat16)
        update_list[layer_idx] = jnp.broadcast_to(combined[None], (replicas, row_count, columns))
    return (jnp.stack(moment_list), jnp.stack(update_list))
```

```python
import functools
import math

import jax
import jax.numpy as jnp
import numpy as np
from jax import lax
from jax.experimental import pallas as pl
from jax.experimental.pallas import tpu as pltpu
from jax.sharding import PartitionSpec as P

DECAY = 0.999
BLOCK = 64
TILE = 256
F32 = jnp.float32
BF16 = jnp.bfloat16
VMEM = pl.BlockSpec(memory_space=pltpu.VMEM)
NT = (((1,), (1,)), ((), ()))
TN = (((0,), (0,)), ((), ()))
NN = (((1,), (0,)), ((), ()))


def dot(left, right, dims=NN):
    return lax.dot_general(left, right, dims, preferred_element_type=F32)


def dot_full(left, right, dims=NN):
    return lax.dot_general(
        left, right, dims, precision=lax.Precision.HIGHEST, preferred_element_type=F32
    )


def split(value):
    high = value.astype(BF16)
    return high, (value - high.astype(F32)).astype(BF16)


def np_basis():
    freq = np.arange(BLOCK)[:, None]
    position = np.arange(BLOCK)[None, :]
    table = np.cos(math.pi * (position + 0.5) * freq / BLOCK) * math.sqrt(2.0 / BLOCK)
    return np.where(freq == 0, table * math.sqrt(0.5), table)


def np_split(table):
    high = table.astype(np.float32).astype(jnp.bfloat16)
    low = (table - high.astype(np.float64)).astype(np.float32).astype(jnp.bfloat16)
    return high, low


def tables(inverse):
    basis = np_basis()
    left = basis.T if inverse else basis
    right = np.kron(np.eye(TILE // BLOCK), basis if inverse else basis.T)
    left_high, left_low = np_split(left)
    right_high, right_low = np_split(right)
    left_all = np.concatenate([left_high, left_low, left_high], axis=1)
    return [jnp.asarray(left_all), jnp.asarray(right_high), jnp.asarray(right_low)]


def two_sided(value, left_all, right_high, right_low):
    high, low = split(value)
    mid = dot(high, right_high) + dot(low, right_high) + dot(high, right_low)
    high, low = split(mid)
    return dot(left_all, jnp.concatenate([high, high, low], axis=0))


def silu_slope(pre_act):
    sigma_h = 1.0 / (1.0 + jnp.exp(-pre_act))
    return sigma_h * (1.0 + pre_act * (1.0 - sigma_h))


def silu(v):
    return v / (1.0 + jnp.exp(-v))


def grads_kernel(layers, sums_ref, x_ref, g_ref, w_ref, out_ref):
    tokens, columns = x_ref.shape
    rows = w_ref.shape[0] // layers
    sums = sums_ref[...]

    def of(base, count, layer):
        return sums[base : base + count, layer * rows : (layer + 1) * rows]

    def gram(m, l):
        return of(2 * tokens + m * rows, rows, l)

    pre, acts = [], []
    for l in range(layers):
        h = of(0, tokens, l)
        for m in range(l):
            h = h + dot_full(acts[m].astype(F32), gram(m, l))
        pre.append(h)
        acts.append(silu(h).astype(BF16))
    deltas = [None] * layers
    for l in reversed(range(layers)):
        e = of(tokens, tokens, l)
        for m in range(l + 1, layers):
            e = e + dot_full(deltas[m].astype(F32), gram(m, l))
        deltas[l] = (e * silu_slope(pre[l])).astype(BF16)
    a_t = jnp.concatenate([a.astype(F32).T for a in acts], axis=0).astype(BF16)
    d_t = jnp.concatenate([d.astype(F32).T for d in deltas], axis=0).astype(BF16)
    row = lax.broadcasted_iota(jnp.int32, (layers * rows, layers * rows), 0) // rows
    col = lax.broadcasted_iota(jnp.int32, (layers * rows, layers * rows), 1) // rows
    a_d = dot(a_t, d_t, NT)
    d_a = dot(d_t, a_t, NT)
    cross = jnp.where(col > row, a_d, jnp.where(col < row, d_a, 0.0))
    cross_high, cross_low = split(cross)

    def body(i, carry):
        at = pl.ds(pl.multiple_of(i * TILE, TILE), TILE)
        w = w_ref[:, at]
        total = dot(a_t, g_ref[:, at]) + dot(d_t, x_ref[:, at])
        total = total + dot(cross_high, w) + dot(cross_low, w)
        out_ref[:, at] = total.astype(BF16)
        return carry

    lax.fori_loop(0, columns // TILE, body, 0)


def encode_kernel(momentum_ref, grad_ref, index_ref, fl, frh, frl, il, irh, irl, out_ref, kept_ref):
    columns = momentum_ref.shape[1]
    per = TILE // BLOCK
    entries = index_ref.shape[1]
    forward = (fl[...], frh[...], frl[...])
    inverse = (il[...], irh[...], irl[...])
    lane_block = lax.broadcasted_iota(jnp.int32, (1, entries), 1) // (entries // per)
    k_iota = lax.broadcasted_iota(jnp.int32, (BLOCK, entries), 0)
    j_iota = lax.broadcasted_iota(jnp.int32, (TILE, entries), 0)

    def body(i, carry):
        at = pl.ds(pl.multiple_of(i * TILE, TILE), TILE)
        fresh = DECAY * momentum_ref[:, at].astype(F32) + grad_ref[:, at].astype(F32)
        coef = two_sided(fresh, *forward)
        index = index_ref[pl.ds(i, 1), :]
        k_hot = jnp.where(k_iota == index >> 6, 1.0, 0.0)
        j_hot = jnp.where(j_iota == (index & 63) + lane_block * BLOCK, 1.0, 0.0).astype(BF16)
        mask = dot(k_hot.astype(BF16), j_hot, NT)
        picked = dot(coef.astype(BF16), j_hot)
        kept_ref[pl.ds(i, 1), :] = jnp.sum(picked * k_hot, axis=0, keepdims=True)
        out_ref[:, at] = (fresh - two_sided(coef * mask, *inverse)).astype(BF16)
        return carry

    lax.fori_loop(0, columns // TILE, body, 0)


def decode_kernel(kept_ref, index_ref, il, irh, irl, out_ref):
    columns = out_ref.shape[1]
    per = TILE // BLOCK
    entries = index_ref.shape[2]
    inverse = (il[...], irh[...], irl[...])
    iota = lax.broadcasted_iota(jnp.int32, (BLOCK, entries), 0)

    def body(i, carry):
        at = pl.ds(pl.multiple_of(i * TILE, TILE), TILE)
        indices = index_ref[i]
        values = kept_ref[i].astype(F32)
        blocks = []
        for b in range(per):
            index = indices[b : b + 1, :]
            kept = values[b : b + 1, :]
            k_hot = jnp.where(iota == index >> 6, kept, 0.0).astype(BF16)
            j_hot = jnp.where(iota == (index & 63), 1.0, 0.0).astype(BF16)
            blocks.append(dot(k_hot, j_hot, NT))
        out_ref[:, at] = two_sided(jnp.concatenate(blocks, axis=1), *inverse).astype(BF16)
        return carry

    lax.fori_loop(0, columns // TILE, body, 0)


def call(kernel, out_shape, *args):
    return pl.pallas_call(
        kernel,
        out_shape=out_shape,
        in_specs=[VMEM] * len(args),
        out_specs=jax.tree.map(lambda _: VMEM, out_shape),
        cost_estimate=pl.CostEstimate(flops=10**9, bytes_accessed=4 * 2**20, transcendentals=0),
    )(*args)


def shifts(axis):
    count = lax.axis_size(axis)
    for step in range(1, count):
        yield step, [(source, (source + step) % count) for source in range(count)]


def exchange(parts, own, axis="section"):
    count = lax.axis_size(axis)
    me = lax.axis_index(axis)
    stacked = jnp.broadcast_to(own[None], (count,) + own.shape)
    for step, pairs in shifts(axis):
        got = lax.ppermute(parts((me + step) % count), axis, pairs)
        source = (me + count - step) % count
        if count == 2:
            slot = lax.broadcasted_iota(jnp.int32, (count,) + (1,) * own.ndim, 0)
            stacked = jnp.where(slot == source, got[None], stacked)
        else:
            stacked = lax.dynamic_update_index_in_dim(stacked, got, source, 0)
    return stacked


def local(inputs, cotangent, weights, momentum, keep_index):
    layers = lax.axis_size("section")
    replicas = lax.axis_size("dp")
    me = lax.axis_index("section")
    rows, width = weights.shape[1:]
    columns = inputs.shape[1]
    groups, kept_count = keep_index.shape[2:]
    weight = weights[0]
    per = TILE // BLOCK

    index_all = lax.all_gather(keep_index[0, 0], "dp")
    index_all = index_all.transpose(1, 0, 2).reshape(groups // per, per, replicas * kept_count)

    def columns_of(i):
        return lax.dynamic_slice_in_dim(weight, i * columns, columns, 1)

    window = exchange(columns_of, columns_of(me)).reshape(layers * rows, columns)
    stack = jnp.concatenate([inputs, cotangent, window], axis=0)
    sums = lax.dot_general(stack, window, NT, preferred_element_type=F32)
    total = sums
    for _, pairs in shifts("section"):
        total = total + lax.ppermute(sums, "section", pairs)

    grads = call(
        functools.partial(grads_kernel, layers),
        jax.ShapeDtypeStruct((layers * rows, columns), BF16),
        total, inputs, cotangent, window,
    ).reshape(layers, rows, columns)

    def grad_of(i):
        return lax.dynamic_index_in_dim(grads, i, 0, keepdims=False)

    grad = exchange(grad_of, grad_of(me)).transpose(1, 0, 2).reshape(rows, width)
    index = keep_index[0, 0].reshape(groups // per, per * kept_count)
    inverse = tables(True)
    momentum_out, kept = call(
        encode_kernel,
        (
            jax.ShapeDtypeStruct((rows, width), BF16),
            jax.ShapeDtypeStruct((groups // per, per * kept_count), F32),
        ),
        momentum[0, 0], grad, index, *tables(False), *inverse,
    )
    kept_all = lax.all_gather(kept.astype(BF16), "dp")
    kept_all = kept_all.reshape(replicas, groups, kept_count).transpose(1, 0, 2)
    update = call(
        decode_kernel,
        jax.ShapeDtypeStruct((rows, width), BF16),
        kept_all.reshape(index_all.shape), index_all, *inverse,
    )
    return momentum_out[None, None], update[None, None]


def solution(mesh):
    return jax.shard_map(
        local,
        mesh=mesh,
        in_specs=(
            P("dp", "section"),
            P("dp", "section"),
            P("section", None, None),
            P("section", "dp", None, None),
            P("section", "dp", None, None),
        ),
        out_specs=(P("section", "dp", None, None), P("section", "dp", None, None)),
        check_vma=False,
    )
```

```python
import functools
import math

import jax
import jax.numpy as jnp
import numpy as np
from jax import lax
from jax.experimental import pallas as pl
from jax.experimental.pallas import tpu as pltpu
from jax.sharding import PartitionSpec as P

DECAY = 0.999
BLOCK = 64
TILE = 256
F32 = jnp.float32
BF16 = jnp.bfloat16
VMEM = pl.BlockSpec(memory_space=pltpu.VMEM)
NT = (((1,), (1,)), ((), ()))
TN = (((0,), (0,)), ((), ()))
NN = (((1,), (0,)), ((), ()))


def dot(left, right, dims=NN):
    return lax.dot_general(left, right, dims, preferred_element_type=F32)


def dot_full(left, right, dims=NN):
    return lax.dot_general(
        left, right, dims, precision=lax.Precision.HIGHEST, preferred_element_type=F32
    )


def split(value):
    high = value.astype(BF16)
    return high, (value - high.astype(F32)).astype(BF16)


def np_basis():
    freq = np.arange(BLOCK)[:, None]
    position = np.arange(BLOCK)[None, :]
    table = np.cos(math.pi * (position + 0.5) * freq / BLOCK) * math.sqrt(2.0 / BLOCK)
    return np.where(freq == 0, table * math.sqrt(0.5), table)


def np_split(table):
    high = table.astype(np.float32).astype(jnp.bfloat16)
    low = (table - high.astype(np.float64)).astype(np.float32).astype(jnp.bfloat16)
    return high, low


def tables(inverse):
    basis = np_basis()
    left = basis.T if inverse else basis
    right = np.kron(np.eye(TILE // BLOCK), basis if inverse else basis.T)
    left_high, left_low = np_split(left)
    right_high, right_low = np_split(right)
    left_all = np.concatenate([left_high, left_low, left_high], axis=1)
    return [jnp.asarray(left_all), jnp.asarray(right_high), jnp.asarray(right_low)]


def two_sided(values, left_all, right_high, right_low):
    high, low = split(jnp.concatenate(values, axis=0))
    mid = dot(high, right_high) + dot(low, right_high) + dot(high, right_low)
    high, low = split(mid)
    outs = []
    for u in range(len(values)):
        h, l = high[u * BLOCK : (u + 1) * BLOCK], low[u * BLOCK : (u + 1) * BLOCK]
        outs.append(dot(left_all, jnp.concatenate([h, h, l], axis=0)))
    return outs


def silu_slope(pre_act):
    sigma_h = 1.0 / (1.0 + jnp.exp(-pre_act))
    return sigma_h * (1.0 + pre_act * (1.0 - sigma_h))


def silu(v):
    return v / (1.0 + jnp.exp(-v))


def grads_kernel(layers, sums_ref, x_ref, g_ref, w_ref, out_ref):
    tokens, columns = x_ref.shape
    rows = w_ref.shape[0] // layers
    sums = sums_ref[...]

    def of(base, count, layer):
        return sums[base : base + count, layer * rows : (layer + 1) * rows]

    def gram(m, l):
        return of(2 * tokens + m * rows, rows, l)

    pre, acts = [], []
    for l in range(layers):
        h = of(0, tokens, l)
        for m in range(l):
            h = h + dot_full(acts[m].astype(F32), gram(m, l))
        pre.append(h)
        acts.append(silu(h).astype(BF16))
    deltas = [None] * layers
    for l in reversed(range(layers)):
        e = of(tokens, tokens, l)
        for m in range(l + 1, layers):
            e = e + dot_full(deltas[m].astype(F32), gram(m, l))
        deltas[l] = (e * silu_slope(pre[l])).astype(BF16)
    a_t = jnp.concatenate([a.astype(F32).T for a in acts], axis=0).astype(BF16)
    d_t = jnp.concatenate([d.astype(F32).T for d in deltas], axis=0).astype(BF16)
    row = lax.broadcasted_iota(jnp.int32, (layers * rows, layers * rows), 0) // rows
    col = lax.broadcasted_iota(jnp.int32, (layers * rows, layers * rows), 1) // rows
    a_d = dot(a_t, d_t, NT)
    d_a = dot(d_t, a_t, NT)
    cross = jnp.where(col > row, a_d, jnp.where(col < row, d_a, 0.0))
    cross_high, cross_low = split(cross)

    step = math.gcd(4 * TILE, columns)

    def body(i, carry):
        at = pl.ds(pl.multiple_of(i * step, step), step)
        w = w_ref[:, at]
        total = dot(a_t, g_ref[:, at]) + dot(d_t, x_ref[:, at])
        total = total + dot(cross_high, w) + dot(cross_low, w)
        out_ref[:, at] = total.astype(BF16)
        return carry

    lax.fori_loop(0, columns // step, body, 0)


def encode_tiles(count, first, momentum_at, grad_at, index_ref, table_refs, store):
    per = TILE // BLOCK
    entries = index_ref.shape[1]
    forward = [ref[...] for ref in table_refs[:3]]
    inverse = [ref[...] for ref in table_refs[3:]]
    lane_block = lax.broadcasted_iota(jnp.int32, (1, entries), 1) // (entries // per)
    k_iota = lax.broadcasted_iota(jnp.int32, (BLOCK, entries), 0)
    j_iota = lax.broadcasted_iota(jnp.int32, (TILE, entries), 0)
    unroll = math.gcd(8, count)

    def body(n, carry):
        tiles = [n * unroll + u for u in range(unroll)]
        fresh = [DECAY * momentum_at(i).astype(F32) + grad_at(i).astype(F32) for i in tiles]
        coefs = two_sided(fresh, *forward)
        masked, rows = [], []
        for i, coef in zip(tiles, coefs):
            index = index_ref[pl.ds(first + i, 1), :]
            k_hot = jnp.where(k_iota == index >> 6, 1.0, 0.0)
            j_at = (index & 63) + lane_block * BLOCK
            j_hot = jnp.where(j_iota == j_at, 1.0, 0.0).astype(BF16)
            mask = dot(k_hot.astype(BF16), j_hot, NT)
            picked = dot(coef.astype(BF16), j_hot)
            rows.append(jnp.sum(picked * k_hot, axis=0, keepdims=True))
            masked.append(coef * mask)
        fields = two_sided(masked, *inverse)
        for i, row, old, field in zip(tiles, rows, fresh, fields):
            store(i, (old - field).astype(BF16), row)
        return carry

    lax.fori_loop(0, count // unroll, body, 0)


def tile_at(start):
    return pl.ds(pl.multiple_of(start, TILE), TILE)


def encode_own(momentum_ref, grad_ref, index_ref, *refs):
    table_refs, (out_ref, kept_ref) = refs[:6], refs[6:]
    columns = grad_ref.shape[1]
    count = columns // TILE
    first = lax.axis_index("section") * count

    def store(i, value, row):
        out_ref[:, tile_at(i * TILE)] = value
        kept_ref[pl.ds(i, 1), :] = row

    encode_tiles(
        count, first, lambda i: momentum_ref[:, tile_at((first + i) * TILE)],
        lambda i: grad_ref[:, tile_at(i * TILE)], index_ref, table_refs, store,
    )


def encode_rest(sections, momentum_ref, own_ref, own_kept_ref, index_ref, *refs):
    grad_refs, refs = refs[: sections - 1], refs[sections - 1 :]
    table_refs, (out_ref, kept_ref) = refs[:6], refs[6:]
    columns = own_ref.shape[1]
    count = columns // TILE
    me = lax.axis_index("section")

    def copy(i, carry):
        out_ref[:, tile_at((me * count + i) * TILE)] = own_ref[:, tile_at(i * TILE)]
        kept_ref[pl.ds(me * count + i, 1), :] = own_kept_ref[pl.ds(i, 1), :]
        return carry

    lax.fori_loop(0, count, copy, 0)
    for step, grad_ref in enumerate(grad_refs, 1):
        first = lax.rem(me + sections - step, sections) * count

        def store(i, value, row, first=first):
            out_ref[:, tile_at((first + i) * TILE)] = value
            kept_ref[pl.ds(first + i, 1), :] = row

        encode_tiles(
            count, first, lambda i: momentum_ref[:, tile_at((first + i) * TILE)],
            lambda i: grad_ref[:, tile_at(i * TILE)], index_ref, table_refs, store,
        )


def decode_kernel(kept_ref, k_ref, j_ref, il, irh, irl, out_ref):
    columns = out_ref.shape[1]
    per = TILE // BLOCK
    entries = k_ref.shape[2]
    inverse = (il[...], irh[...], irl[...])
    iota = lax.broadcasted_iota(jnp.int32, (BLOCK, entries), 0).astype(F32).astype(BF16)
    zero, one = jnp.zeros((), BF16), jnp.ones((), BF16)
    unroll = math.gcd(4, columns // TILE)

    def body(n, carry):
        sums = []
        for u in range(unroll):
            i = n * unroll + u
            ks, js, values = k_ref[i], j_ref[i], kept_ref[i]
            blocks = []
            for b in range(per):
                k_hot = jnp.where(iota == ks[b : b + 1, :], values[b : b + 1, :], zero)
                j_hot = jnp.where(iota == js[b : b + 1, :], one, zero)
                blocks.append(dot(k_hot, j_hot, NT))
            sums.append(jnp.concatenate(blocks, axis=1))
        for u, field in enumerate(two_sided(sums, *inverse)):
            out_ref[:, tile_at((n * unroll + u) * TILE)] = field.astype(BF16)
        return carry

    lax.fori_loop(0, columns // TILE // unroll, body, 0)


MESH = pl.DeviceIdType.MESH


def gather_kernel(value_ref, out_ref, send_sem, recv_sem):
    count = out_ref.shape[0]
    me = lax.axis_index("dp")
    section = lax.axis_index("section")
    barrier = pltpu.get_barrier_semaphore()
    peers = [lax.rem(me + k, count) for k in range(1, count)]
    for peer in peers:
        pl.semaphore_signal(barrier, inc=1, device_id=(section, peer), device_id_type=MESH)
    pl.semaphore_wait(barrier, count - 1)
    copies = []
    for k, peer in enumerate(peers):
        copies.append(
            pltpu.make_async_remote_copy(
                src_ref=value_ref, dst_ref=out_ref.at[me],
                send_sem=send_sem.at[k], recv_sem=recv_sem.at[k],
                device_id=(section, peer), device_id_type=MESH,
            )
        )
        copies[-1].start()
    out_ref[me] = value_ref[...]
    for copy in copies:
        copy.wait()


def gather(value, collective_id):
    count = lax.axis_size("dp")
    return pl.pallas_call(
        gather_kernel,
        out_shape=jax.ShapeDtypeStruct((count,) + value.shape, value.dtype),
        in_specs=[VMEM],
        out_specs=VMEM,
        scratch_shapes=[pltpu.SemaphoreType.DMA((count - 1,)), pltpu.SemaphoreType.DMA((count - 1,))],
        compiler_params=pltpu.CompilerParams(collective_id=collective_id, has_side_effects=True),
    )(value)


def window_kernel(sections, weight_ref, index_ref, out_ref, index_out, local_sem, send_sem, recv_sem,
                  pass_send, pass_recv, index_send, index_recv):
    count = index_out.shape[0]
    half = out_ref.shape[2] // 2
    columns = 2 * half
    me, section = lax.axis_index("dp"), lax.axis_index("section")
    twin = me + 1 - 2 * lax.rem(me, 2)
    mine = lax.rem(me, 2)
    others = [lax.rem(section + k, sections) for k in range(1, sections)]
    peers = [lax.rem(me + k, count) for k in range(1, count)]
    barrier = pltpu.get_barrier_semaphore()
    for other in others:
        pl.semaphore_signal(barrier, inc=1, device_id=(other, me), device_id_type=MESH)
    for peer in peers:
        pl.semaphore_signal(barrier, inc=1, device_id=(section, peer), device_id_type=MESH)
    pl.semaphore_wait(barrier, sections + count - 2)
    my_half = pl.ds(pl.multiple_of(mine * half, half), half)
    sends = []
    for k, other in enumerate(others):
        source = pl.ds(pl.multiple_of(other * columns + mine * half, half), half)
        sends.append(
            pltpu.make_async_remote_copy(
                src_ref=weight_ref.at[:, source], dst_ref=out_ref.at[section, :, my_half],
                send_sem=send_sem.at[k], recv_sem=recv_sem.at[k],
                device_id=(other, me), device_id_type=MESH,
            )
        )
        sends[-1].start()
    own = pltpu.make_async_copy(
        weight_ref.at[:, pl.ds(pl.multiple_of(section * columns, columns), columns)],
        out_ref.at[section], local_sem,
    )
    own.start()
    index_copies = []
    for k, peer in enumerate(peers):
        index_copies.append(
            pltpu.make_async_remote_copy(
                src_ref=index_ref, dst_ref=index_out.at[me],
                send_sem=index_send.at[k], recv_sem=index_recv.at[k],
                device_id=(section, peer), device_id_type=MESH,
            )
        )
        index_copies[-1].start()
    index_out[me] = index_ref[...]
    passes = []
    for k, send in enumerate(sends):
        send.wait_recv()
        layer = lax.rem(section + sections - 1 - k, sections)
        passes.append(
            pltpu.make_async_remote_copy(
                src_ref=out_ref.at[layer, :, my_half], dst_ref=out_ref.at[layer, :, my_half],
                send_sem=pass_send.at[k], recv_sem=pass_recv.at[k],
                device_id=(section, twin), device_id_type=MESH,
            )
        )
        passes[-1].start()
    for copy in passes + index_copies:
        copy.wait()
    for send in sends:
        send.wait_send()
    own.wait()


def windows(weight, index, sections, collective_id):
    count = lax.axis_size("dp")
    dma = pltpu.SemaphoreType.DMA
    rows, width = weight.shape
    return pl.pallas_call(
        functools.partial(window_kernel, sections),
        out_shape=(
            jax.ShapeDtypeStruct((sections, rows, width // sections), weight.dtype),
            jax.ShapeDtypeStruct((count,) + index.shape, index.dtype),
        ),
        in_specs=[VMEM, VMEM],
        out_specs=(VMEM, VMEM),
        scratch_shapes=[dma] + [dma((sections - 1,))] * 4 + [dma((count - 1,))] * 2,
        compiler_params=pltpu.CompilerParams(collective_id=collective_id, has_side_effects=True),
    )(weight, index)


def call(kernel, out_shape, *args):
    return pl.pallas_call(
        kernel,
        out_shape=out_shape,
        in_specs=[VMEM] * len(args),
        out_specs=jax.tree.map(lambda _: VMEM, out_shape),
        cost_estimate=pl.CostEstimate(flops=10**9, bytes_accessed=4 * 2**20, transcendentals=0),
    )(*args)


def shifts(axis):
    count = lax.axis_size(axis)
    for step in range(1, count):
        yield step, [(source, (source + step) % count) for source in range(count)]


def local(inputs, cotangent, weights, momentum, keep_index):
    sections = lax.axis_size("section")
    replicas = lax.axis_size("dp")
    me = lax.axis_index("section")
    rows, width = weights.shape[1:]
    columns = inputs.shape[1]
    groups, kept_count = keep_index.shape[2:]
    per = TILE // BLOCK
    tiles = groups // per
    index = keep_index[0, 0].reshape(tiles, per * kept_count)

    def by_block(value):
        value = value.reshape(replicas, groups, kept_count).transpose(1, 0, 2)
        return value.reshape(tiles, per, replicas * kept_count)

    window, index_all = windows(weights[0], index, sections, 0)
    window = window.reshape(sections * rows, columns)
    stack = jnp.concatenate([inputs, cotangent, window], axis=0)
    sums = lax.dot_general(stack, window, NT, preferred_element_type=F32)
    total = sums
    for _, pairs in shifts("section"):
        total = total + lax.ppermute(sums, "section", pairs)

    grads = call(
        functools.partial(grads_kernel, sections),
        jax.ShapeDtypeStruct((sections * rows, columns), BF16),
        total, inputs, cotangent, window,
    ).reshape(sections, rows, columns)

    def grad_of(i):
        return lax.dynamic_index_in_dim(grads, i, 0, keepdims=False)

    received = [
        lax.ppermute(grad_of((me + step) % sections), "section", pairs)
        for step, pairs in shifts("section")
    ]
    inverse = tables(True)
    every = tables(False) + inverse
    own_tiles = columns // TILE
    own_out, own_kept = call(
        encode_own,
        (
            jax.ShapeDtypeStruct((rows, columns), BF16),
            jax.ShapeDtypeStruct((own_tiles, per * kept_count), F32),
        ),
        momentum[0, 0], grad_of(me), index, *every,
    )
    index_all = by_block(index_all)
    k_all = (index_all >> 6).astype(F32).astype(BF16)
    j_all = (index_all & 63).astype(F32).astype(BF16)
    momentum_out, kept = call(
        functools.partial(encode_rest, sections),
        (
            jax.ShapeDtypeStruct((rows, width), BF16),
            jax.ShapeDtypeStruct((tiles, per * kept_count), F32),
        ),
        momentum[0, 0], own_out, own_kept, index, *received, *every,
    )
    kept_all = by_block(gather(kept.astype(BF16), 1))
    update = call(
        decode_kernel,
        jax.ShapeDtypeStruct((rows, width), BF16),
        kept_all, k_all, j_all, *inverse,
    )
    return momentum_out[None, None], update[None, None]


def solution(mesh):
    return jax.shard_map(
        local,
        mesh=mesh,
        in_specs=(
            P("dp", "section"),
            P("dp", "section"),
            P("section", None, None),
            P("section", "dp", None, None),
            P("section", "dp", None, None),
        ),
        out_specs=(P("section", "dp", None, None), P("section", "dp", None, None)),
        check_vma=False,
    )
```

```python
import functools
import math

import jax
import jax.numpy as jnp
import numpy as np
from jax import lax
from jax.experimental import pallas as pl
from jax.experimental.pallas import tpu as pltpu
from jax.sharding import PartitionSpec as P

DECAY = 0.999
BLOCK = 64
TILE = 256
F32 = jnp.float32
BF16 = jnp.bfloat16
VMEM = pl.BlockSpec(memory_space=pltpu.VMEM)
NT = (((1,), (1,)), ((), ()))
TN = (((0,), (0,)), ((), ()))
NN = (((1,), (0,)), ((), ()))


def dot(left, right, dims=NN):
    return lax.dot_general(left, right, dims, preferred_element_type=F32)


def dot_full(left, right, dims=NN):
    return lax.dot_general(
        left, right, dims, precision=lax.Precision.HIGHEST, preferred_element_type=F32
    )


def split(value):
    high = value.astype(BF16)
    return high, (value - high.astype(F32)).astype(BF16)


def np_basis():
    freq = np.arange(BLOCK)[:, None]
    position = np.arange(BLOCK)[None, :]
    table = np.cos(math.pi * (position + 0.5) * freq / BLOCK) * math.sqrt(2.0 / BLOCK)
    return np.where(freq == 0, table * math.sqrt(0.5), table)


def np_split(table):
    high = table.astype(np.float32).astype(jnp.bfloat16)
    low = (table - high.astype(np.float64)).astype(np.float32).astype(jnp.bfloat16)
    return high, low


def tables(inverse):
    basis = np_basis()
    left = basis.T if inverse else basis
    right = np.kron(np.eye(TILE // BLOCK), basis if inverse else basis.T)
    left_high, left_low = np_split(left)
    right_high, right_low = np_split(right)
    left_all = np.concatenate([left_high, left_low, left_high], axis=1)
    return [jnp.asarray(left_all), jnp.asarray(right_high), jnp.asarray(right_low)]


def two_sided(values, left_all, right_high, right_low):
    high, low = split(jnp.concatenate(values, axis=0))
    mid = dot(high, right_high) + dot(low, right_high) + dot(high, right_low)
    high, low = split(mid)
    outs = []
    for u in range(len(values)):
        h, l = high[u * BLOCK : (u + 1) * BLOCK], low[u * BLOCK : (u + 1) * BLOCK]
        outs.append(dot(left_all, jnp.concatenate([h, h, l], axis=0)))
    return outs


def silu_slope(pre_act):
    sigma_h = 1.0 / (1.0 + jnp.exp(-pre_act))
    return sigma_h * (1.0 + pre_act * (1.0 - sigma_h))


def silu(v):
    return v / (1.0 + jnp.exp(-v))


def grads_kernel(layers, sums_ref, got_ref, x_ref, g_ref, w_ref, *refs):
    out_refs, lhs_ref = refs[:layers], refs[layers]
    tokens, columns = x_ref.shape
    rows = w_ref.shape[0] // layers
    sums = sums_ref[...] + got_ref[...].astype(F32)

    def of(base, count, layer):
        return sums[base : base + count, layer * rows : (layer + 1) * rows]

    def gram(m, l):
        return of(2 * tokens + m * rows, rows, l)

    pre, acts = [], []
    for l in range(layers):
        h = of(0, tokens, l)
        for m in range(l):
            h = h + dot_full(acts[m].astype(F32), gram(m, l))
        pre.append(h)
        acts.append(silu(h).astype(BF16))
    deltas = [None] * layers
    for l in reversed(range(layers)):
        e = of(tokens, tokens, l)
        for m in range(l + 1, layers):
            e = e + dot_full(deltas[m].astype(F32), gram(m, l))
        deltas[l] = (e * silu_slope(pre[l])).astype(BF16)
    a_t = jnp.concatenate([a.astype(F32).T for a in acts], axis=0).astype(BF16)
    d_t = jnp.concatenate([d.astype(F32).T for d in deltas], axis=0).astype(BF16)
    row = lax.broadcasted_iota(jnp.int32, (layers * rows, layers * rows), 0) // rows
    col = lax.broadcasted_iota(jnp.int32, (layers * rows, layers * rows), 1) // rows
    a_d = dot(a_t, d_t, NT)
    d_a = dot(d_t, a_t, NT)
    cross = jnp.where(col > row, a_d, jnp.where(col < row, d_a, 0.0))
    cross_high, cross_low = split(cross)

    factors = jnp.concatenate([a_t, d_t, cross_high, cross_low], axis=1)
    for l in range(layers):
        lhs_ref[l] = factors[l * rows : (l + 1) * rows]
    me = lax.axis_index("section")
    turned = [lhs_ref[lax.rem(me + k, layers)] for k in range(layers)]
    factors = jnp.concatenate(turned, axis=0)
    a_t, d_t = factors[:, :tokens], factors[:, tokens : 2 * tokens]
    cross_high = factors[:, 2 * tokens : 2 * tokens + layers * rows]
    cross_low = factors[:, 2 * tokens + layers * rows :]
    step = math.gcd(4 * TILE, columns)

    def body(i, carry):
        at = pl.ds(pl.multiple_of(i * step, step), step)
        w = w_ref[:, at]
        total = dot(a_t, g_ref[:, at]) + dot(d_t, x_ref[:, at])
        total = total + dot(cross_high, w) + dot(cross_low, w)
        for k, out_ref in enumerate(out_refs):
            out_ref[:, at] = total[k * rows : (k + 1) * rows].astype(BF16)
        return carry

    lax.fori_loop(0, columns // step, body, 0)


def encode_tiles(count, first, momentum_at, grad_at, index_ref, table_refs, store):
    per = TILE // BLOCK
    entries = index_ref.shape[1]
    forward = [ref[...] for ref in table_refs[:3]]
    inverse = [ref[...] for ref in table_refs[3:]]
    slot = lax.broadcasted_iota(jnp.int32, (1, entries), 1) // (entries // per)
    lane_block = (slot + per - lax.rem(lax.axis_index("dp"), per)) & (per - 1)
    k_iota = lax.broadcasted_iota(jnp.int32, (BLOCK, entries), 0)
    j_iota = lax.broadcasted_iota(jnp.int32, (TILE, entries), 0)
    unroll = math.gcd(8, count)

    def body(n, carry):
        tiles = [n * unroll + u for u in range(unroll)]
        fresh = [DECAY * momentum_at(i).astype(F32) + grad_at(i).astype(F32) for i in tiles]
        coefs = two_sided(fresh, *forward)
        masked, rows = [], []
        for i, coef in zip(tiles, coefs):
            index = index_ref[pl.ds(first + i, 1), :]
            k_hot = jnp.where(k_iota == index >> 6, 1.0, 0.0)
            j_at = (index & 63) + lane_block * BLOCK
            j_hot = jnp.where(j_iota == j_at, 1.0, 0.0).astype(BF16)
            mask = dot(k_hot.astype(BF16), j_hot, NT)
            picked = dot(coef.astype(BF16), j_hot)
            rows.append(jnp.sum(picked * k_hot, axis=0, keepdims=True))
            masked.append(coef * mask)
        fields = two_sided(masked, *inverse)
        for i, row, old, field in zip(tiles, rows, fresh, fields):
            store(i, (old - field).astype(BF16), row)
        return carry

    lax.fori_loop(0, count // unroll, body, 0)


def tile_at(start):
    return pl.ds(pl.multiple_of(start, TILE), TILE)


def encode_own(momentum_ref, grad_ref, index_ref, *refs):
    table_refs, (out_ref, kept_ref) = refs[:6], refs[6:]
    columns = grad_ref.shape[1]
    count = columns // TILE
    first = lax.axis_index("section") * count

    def store(i, value, row):
        out_ref[:, tile_at(i * TILE)] = value
        kept_ref[pl.ds(i, 1), :] = row

    encode_tiles(
        count, first, lambda i: momentum_ref[:, tile_at((first + i) * TILE)],
        lambda i: grad_ref[:, tile_at(i * TILE)], index_ref, table_refs, store,
    )


def encode_rest(sections, momentum_ref, own_ref, own_kept_ref, index_ref, *refs):
    grad_refs, refs = refs[: sections - 1], refs[sections - 1 :]
    table_refs, (out_ref, rounded_ref, kept_ref) = refs[:6], refs[6:]
    columns = own_ref.shape[1]
    count = columns // TILE
    me = lax.axis_index("section")

    def copy(i, carry):
        out_ref[:, tile_at((me * count + i) * TILE)] = own_ref[:, tile_at(i * TILE)]
        kept_ref[pl.ds(me * count + i, 1), :] = own_kept_ref[pl.ds(i, 1), :]
        return carry

    lax.fori_loop(0, count, copy, 0)
    for step, grad_ref in enumerate(grad_refs, 1):
        first = lax.rem(me + sections - step, sections) * count

        def store(i, value, row, first=first):
            out_ref[:, tile_at((first + i) * TILE)] = value
            kept_ref[pl.ds(first + i, 1), :] = row

        encode_tiles(
            count, first, lambda i: momentum_ref[:, tile_at((first + i) * TILE)],
            lambda i: grad_ref[:, tile_at(i * TILE)], index_ref, table_refs, store,
        )
    rounded_ref[...] = kept_ref[...].astype(BF16)


def decode_kernel(kept_ref, index_ref, il, irh, irl, out_ref):
    columns = out_ref.shape[1]
    per = TILE // BLOCK
    replicas, _, lanes = index_ref.shape
    entries = replicas // per * lanes
    inverse = (il[...], irh[...], irl[...])
    iota = lax.broadcasted_iota(jnp.int32, (BLOCK, entries), 0).astype(F32).astype(BF16)
    zero, one = jnp.zeros((), BF16), jnp.ones((), BF16)
    slot = lax.broadcasted_iota(jnp.int32, (1, lanes), 1) // (lanes // per)
    unroll = math.gcd(4, columns // TILE)

    def merged(rows, b):
        parts = []
        for q in range(0, replicas, per):
            part = rows[q]
            for p in range(1, per):
                part = jnp.where(slot == (b + p) % per, rows[q + p], part)
            parts.append(part)
        return jnp.concatenate(parts, axis=1)

    def body(n, carry):
        sums = []
        for u in range(unroll):
            i = n * unroll + u
            values = [kept_ref[q, pl.ds(i, 1), :] for q in range(replicas)]
            indices = [index_ref[q, pl.ds(i, 1), :] for q in range(replicas)]
            blocks = []
            for b in range(per):
                index = merged(indices, b)
                k_row = (index >> 6).astype(F32).astype(BF16)
                j_row = (index & 63).astype(F32).astype(BF16)
                k_hot = jnp.where(iota == k_row, merged(values, b).astype(BF16), zero)
                j_hot = jnp.where(iota == j_row, one, zero)
                blocks.append(dot(k_hot, j_hot, NT))
            sums.append(jnp.concatenate(blocks, axis=1))
        for u, field in enumerate(two_sided(sums, *inverse)):
            out_ref[:, tile_at((n * unroll + u) * TILE)] = field.astype(BF16)
        return carry

    lax.fori_loop(0, columns // TILE // unroll, body, 0)


MESH = pl.DeviceIdType.MESH


def inner_of(count):
    return math.gcd(4, count)


def neighbours(count):
    inner = inner_of(count)
    me = lax.axis_index("dp")
    place = lax.rem(me, inner)
    base = me - place
    near = [base + lax.rem(place + k, inner) for k in range(1, inner)]
    far = [lax.rem(me + k * inner, count) for k in range(1, count // inner)]
    return me, base, near, far


def gather_near(value_ref, out_ref, send_sem, recv_sem):
    me, _, near, _ = neighbours(out_ref.shape[0])
    section = lax.axis_index("section")
    copies = []
    for k, peer in enumerate(near):
        copies.append(
            pltpu.make_async_remote_copy(
                src_ref=value_ref, dst_ref=out_ref.at[me],
                send_sem=send_sem.at[k], recv_sem=recv_sem.at[k],
                device_id=(section, peer), device_id_type=MESH,
            )
        )
        copies[-1].start()
    return copies


def gather_far(out_ref, send_sem, recv_sem):
    _, base, near, far = neighbours(out_ref.shape[0])
    section = lax.axis_index("section")
    group = out_ref.at[pl.ds(base, len(near) + 1)]
    copies = []
    for k, peer in enumerate(far):
        copies.append(
            pltpu.make_async_remote_copy(
                src_ref=group, dst_ref=group,
                send_sem=send_sem.at[len(near) + k], recv_sem=recv_sem.at[len(near) + k],
                device_id=(section, peer), device_id_type=MESH,
            )
        )
        copies[-1].start()
    return copies


def gather_count(count):
    inner = inner_of(count)
    return inner - 1 + count // inner - 1


def gather_kernel(value_ref, out_ref, own_sem, send_sem, recv_sem):
    me, _, near, far = neighbours(out_ref.shape[0])
    section = lax.axis_index("section")
    barrier = pltpu.get_barrier_semaphore()
    for peer in near + far:
        pl.semaphore_signal(barrier, inc=1, device_id=(section, peer), device_id_type=MESH)
    own = pltpu.make_async_copy(value_ref, out_ref.at[me], own_sem)
    own.start()
    pl.semaphore_wait(barrier, len(near) + len(far))
    copies = gather_near(value_ref, out_ref, send_sem, recv_sem)
    own.wait()
    for copy in copies:
        copy.wait()
    for copy in gather_far(out_ref, send_sem, recv_sem):
        copy.wait()


def gather(value, collective_id):
    count = lax.axis_size("dp")
    dma = pltpu.SemaphoreType.DMA
    return pl.pallas_call(
        gather_kernel,
        out_shape=jax.ShapeDtypeStruct((count,) + value.shape, value.dtype),
        in_specs=[VMEM],
        out_specs=VMEM,
        scratch_shapes=[dma] + [dma((gather_count(count),))] * 2,
        compiler_params=pltpu.CompilerParams(collective_id=collective_id, has_side_effects=True),
    )(value)


CHUNKS = 2


def window_kernel(sections, weight_ref, index_ref, out_ref, index_out, local_sem, own_sem, send_sem, recv_sem,
                  pass_send, pass_recv, index_send, index_recv):
    half = out_ref.shape[2] // 2
    columns = 2 * half
    piece = out_ref.shape[1] // CHUNKS
    me, _, near, far = neighbours(index_out.shape[0])
    section = lax.axis_index("section")
    twin = me + 1 - 2 * lax.rem(me, 2)
    mine = lax.rem(me, 2)
    others = [lax.rem(section + k, sections) for k in range(1, sections)]
    barrier = pltpu.get_barrier_semaphore()
    for other in others:
        pl.semaphore_signal(barrier, inc=1, device_id=(other, me), device_id_type=MESH)
    for peer in near + far:
        pl.semaphore_signal(barrier, inc=1, device_id=(section, peer), device_id_type=MESH)
    own = pltpu.make_async_copy(
        weight_ref.at[:, pl.ds(pl.multiple_of(section * columns, columns), columns)],
        out_ref.at[section], local_sem,
    )
    own.start()
    own_index = pltpu.make_async_copy(index_ref, index_out.at[me], own_sem)
    own_index.start()
    pl.semaphore_wait(barrier, len(others) + len(near) + len(far))
    my_half = pl.ds(pl.multiple_of(mine * half, half), half)
    sends = []
    for c in range(CHUNKS):
        lines = pl.ds(c * piece, piece)
        for k, other in enumerate(others):
            source = pl.ds(pl.multiple_of(other * columns + mine * half, half), half)
            sends.append(
                pltpu.make_async_remote_copy(
                    src_ref=weight_ref.at[lines, source], dst_ref=out_ref.at[section, lines, my_half],
                    send_sem=send_sem.at[len(sends)], recv_sem=recv_sem.at[len(sends)],
                    device_id=(other, me), device_id_type=MESH,
                )
            )
            sends[-1].start()
    index_copies = gather_near(index_ref, index_out, index_send, index_recv)
    own_index.wait()
    for copy in index_copies:
        copy.wait()
    waiting = gather_far(index_out, index_send, index_recv)
    for n, send in enumerate(sends):
        send.wait_recv()
        layer = lax.rem(section + sections - 1 - n % (sections - 1), sections)
        lines = pl.ds(n // (sections - 1) * piece, piece)
        half_ref = out_ref.at[layer, lines, my_half]
        waiting.append(
            pltpu.make_async_remote_copy(
                src_ref=half_ref, dst_ref=half_ref,
                send_sem=pass_send.at[n], recv_sem=pass_recv.at[n],
                device_id=(section, twin), device_id_type=MESH,
            )
        )
        waiting[-1].start()
    for copy in waiting:
        copy.wait()
    for send in sends:
        send.wait_send()
    own.wait()


def windows(weight, index, sections, collective_id):
    count = lax.axis_size("dp")
    dma = pltpu.SemaphoreType.DMA
    rows, width = weight.shape
    return pl.pallas_call(
        functools.partial(window_kernel, sections),
        out_shape=(
            jax.ShapeDtypeStruct((sections, rows, width // sections), weight.dtype),
            jax.ShapeDtypeStruct((count,) + index.shape, index.dtype),
        ),
        in_specs=[VMEM, VMEM],
        out_specs=(VMEM, VMEM),
        scratch_shapes=[dma] * 2 + [dma(((sections - 1) * CHUNKS,))] * 4 + [dma((gather_count(count),))] * 2,
        compiler_params=pltpu.CompilerParams(collective_id=collective_id, has_side_effects=True),
    )(weight, index)


def call(kernel, out_shape, *args, scratch=()):
    return pl.pallas_call(
        kernel,
        out_shape=out_shape,
        in_specs=[VMEM] * len(args),
        out_specs=jax.tree.map(lambda _: VMEM, out_shape),
        scratch_shapes=scratch,
        cost_estimate=pl.CostEstimate(flops=10**9, bytes_accessed=4 * 2**20, transcendentals=0),
    )(*args)


def shifts(axis):
    count = lax.axis_size(axis)
    for step in range(1, count):
        yield step, [(source, (source + step) % count) for source in range(count)]


def local(inputs, cotangent, weights, momentum, keep_index):
    sections = lax.axis_size("section")
    replicas = lax.axis_size("dp")
    me = lax.axis_index("section")
    rows, width = weights.shape[1:]
    columns = inputs.shape[1]
    groups, kept_count = keep_index.shape[2:]
    per = TILE // BLOCK
    tiles = groups // per
    index = keep_index[0, 0].reshape(tiles, per * kept_count)
    index = jnp.roll(index, lax.axis_index("dp") % per * kept_count, axis=1)

    window, index_all = windows(weights[0], index, sections, 0)
    window = window.reshape(sections * rows, columns)
    stack = jnp.concatenate([inputs, cotangent, window], axis=0)
    sums = lax.dot_general(stack, window, NT, preferred_element_type=F32)
    rounded = sums.astype(BF16)
    got = [lax.ppermute(rounded, "section", pairs) for _, pairs in shifts("section")]
    got = functools.reduce(jnp.add, [part.astype(F32) for part in got]) if len(got) > 1 else got[0]
    depth = 2 * (inputs.shape[0] + sections * rows)
    grads = call(
        functools.partial(grads_kernel, sections),
        [jax.ShapeDtypeStruct((rows, columns), BF16)] * sections,
        sums, got, inputs, cotangent, window,
        scratch=[pltpu.VMEM((sections, rows, depth), BF16)],
    )
    received = [
        lax.ppermute(grads[step], "section", pairs) for step, pairs in shifts("section")
    ]
    inverse = tables(True)
    every = tables(False) + inverse
    own_tiles = columns // TILE
    own_out, own_kept = call(
        encode_own,
        (
            jax.ShapeDtypeStruct((rows, columns), BF16),
            jax.ShapeDtypeStruct((own_tiles, per * kept_count), F32),
        ),
        momentum[0, 0], grads[0], index, *every,
    )
    momentum_out, kept = call(
        functools.partial(encode_rest, sections),
        (
            jax.ShapeDtypeStruct((rows, width), BF16),
            jax.ShapeDtypeStruct((tiles, per * kept_count), BF16),
        ),
        momentum[0, 0], own_out, own_kept, index, *received, *every,
        scratch=[pltpu.VMEM((tiles, per * kept_count), F32)],
    )
    kept_all = gather(kept, 1).astype(F32)
    update = call(
        decode_kernel,
        jax.ShapeDtypeStruct((rows, width), BF16),
        kept_all, index_all, *inverse,
    )
    return momentum_out[None, None], update[None, None]


def solution(mesh):
    return jax.shard_map(
        local,
        mesh=mesh,
        in_specs=(
            P("dp", "section"),
            P("dp", "section"),
            P("section", None, None),
            P("section", "dp", None, None),
            P("section", "dp", None, None),
        ),
        out_specs=(P("section", "dp", None, None), P("section", "dp", None, None)),
        check_vma=False,
    )
```

```python
import functools
import math

import jax
import jax.numpy as jnp
import numpy as np
from jax import lax
from jax.experimental import pallas as pl
from jax.experimental.pallas import tpu as pltpu
from jax.sharding import PartitionSpec as P

DECAY = 0.999
BLOCK = 64
TILE = 256
F32 = jnp.float32
BF16 = jnp.bfloat16
VMEM = pl.BlockSpec(memory_space=pltpu.VMEM)
NT = (((1,), (1,)), ((), ()))
TN = (((0,), (0,)), ((), ()))
NN = (((1,), (0,)), ((), ()))


def dot(left, right, dims=NN):
    return lax.dot_general(left, right, dims, preferred_element_type=F32)


def dot_full(left, right, dims=NN):
    return lax.dot_general(
        left, right, dims, precision=lax.Precision.HIGHEST, preferred_element_type=F32
    )


def split(value):
    high = value.astype(BF16)
    return high, (value - high.astype(F32)).astype(BF16)


def np_basis():
    freq = np.arange(BLOCK)[:, None]
    position = np.arange(BLOCK)[None, :]
    table = np.cos(math.pi * (position + 0.5) * freq / BLOCK) * math.sqrt(2.0 / BLOCK)
    return np.where(freq == 0, table * math.sqrt(0.5), table)


def np_split(table):
    high = table.astype(np.float32).astype(jnp.bfloat16)
    low = (table - high.astype(np.float64)).astype(np.float32).astype(jnp.bfloat16)
    return high, low


def tables(inverse):
    basis = np_basis()
    left = basis.T if inverse else basis
    right = np.kron(np.eye(TILE // BLOCK), basis if inverse else basis.T)
    left_high, left_low = np_split(left)
    right_high, right_low = np_split(right)
    left_all = np.concatenate([left_high, left_low, left_high], axis=1)
    return [jnp.asarray(left_all), jnp.asarray(right_high), jnp.asarray(right_low)]


def two_sided(values, left_all, right_high, right_low):
    high, low = split(jnp.concatenate(values, axis=0))
    mid = dot(high, right_high) + dot(low, right_high) + dot(high, right_low)
    high, low = split(mid)
    outs = []
    for u in range(len(values)):
        h, l = high[u * BLOCK : (u + 1) * BLOCK], low[u * BLOCK : (u + 1) * BLOCK]
        outs.append(dot(left_all, jnp.concatenate([h, h, l], axis=0)))
    return outs


def silu_slope(pre_act):
    sigma_h = 1.0 / (1.0 + jnp.exp(-pre_act))
    return sigma_h * (1.0 + pre_act * (1.0 - sigma_h))


def silu(v):
    return v / (1.0 + jnp.exp(-v))


def grads_kernel(layers, sums_ref, got_ref, x_ref, g_ref, w_ref, *refs):
    out_refs, lhs_ref = refs[:layers], refs[layers]
    tokens, columns = x_ref.shape
    rows = w_ref.shape[0] // layers
    sums = sums_ref[...] + got_ref[...].astype(F32)

    def of(base, count, layer):
        return sums[base : base + count, layer * rows : (layer + 1) * rows]

    def gram(m, l):
        return of(2 * tokens + m * rows, rows, l)

    pre, acts = [], []
    for l in range(layers):
        h = of(0, tokens, l)
        for m in range(l):
            h = h + dot_full(acts[m].astype(F32), gram(m, l))
        pre.append(h)
        acts.append(silu(h).astype(BF16))
    deltas = [None] * layers
    for l in reversed(range(layers)):
        e = of(tokens, tokens, l)
        for m in range(l + 1, layers):
            e = e + dot_full(deltas[m].astype(F32), gram(m, l))
        deltas[l] = (e * silu_slope(pre[l])).astype(BF16)
    a_t = jnp.concatenate([a.astype(F32).T for a in acts], axis=0).astype(BF16)
    d_t = jnp.concatenate([d.astype(F32).T for d in deltas], axis=0).astype(BF16)
    row = lax.broadcasted_iota(jnp.int32, (layers * rows, layers * rows), 0) // rows
    col = lax.broadcasted_iota(jnp.int32, (layers * rows, layers * rows), 1) // rows
    a_d = dot(a_t, d_t, NT)
    d_a = dot(d_t, a_t, NT)
    cross = jnp.where(col > row, a_d, jnp.where(col < row, d_a, 0.0))
    cross_high, cross_low = split(cross)

    factors = jnp.concatenate([a_t, d_t, cross_high, cross_low], axis=1)
    for l in range(layers):
        lhs_ref[l] = factors[l * rows : (l + 1) * rows]
    me = lax.axis_index("section")
    turned = [lhs_ref[lax.rem(me + k, layers)] for k in range(layers)]
    factors = jnp.concatenate(turned, axis=0)
    a_t, d_t = factors[:, :tokens], factors[:, tokens : 2 * tokens]
    cross_high = factors[:, 2 * tokens : 2 * tokens + layers * rows]
    cross_low = factors[:, 2 * tokens + layers * rows :]
    step = math.gcd(4 * TILE, columns)

    def body(i, carry):
        at = pl.ds(pl.multiple_of(i * step, step), step)
        w = w_ref[:, at]
        total = dot(a_t, g_ref[:, at]) + dot(d_t, x_ref[:, at])
        total = total + dot(cross_high, w) + dot(cross_low, w)
        for k, out_ref in enumerate(out_refs):
            out_ref[:, at] = total[k * rows : (k + 1) * rows].astype(BF16)
        return carry

    lax.fori_loop(0, columns // step, body, 0)


def encode_tiles(count, first, momentum_at, grad_at, index_ref, table_refs, store):
    per = TILE // BLOCK
    entries = index_ref.shape[1]
    forward = [ref[...] for ref in table_refs[:3]]
    inverse = [ref[...] for ref in table_refs[3:]]
    slot = lax.broadcasted_iota(jnp.int32, (1, entries), 1) // (entries // per)
    lane_block = (slot + per - lax.rem(lax.axis_index("dp"), per)) & (per - 1)
    k_iota = lax.broadcasted_iota(jnp.int32, (BLOCK, entries), 0)
    j_iota = lax.broadcasted_iota(jnp.int32, (TILE, entries), 0)
    unroll = math.gcd(8, count)

    def body(n, carry):
        tiles = [n * unroll + u for u in range(unroll)]
        fresh = [DECAY * momentum_at(i).astype(F32) + grad_at(i).astype(F32) for i in tiles]
        coefs = two_sided(fresh, *forward)
        masked, rows = [], []
        for i, coef in zip(tiles, coefs):
            index = index_ref[pl.ds(first + i, 1), :]
            k_hot = jnp.where(k_iota == index >> 6, 1.0, 0.0)
            j_at = (index & 63) + lane_block * BLOCK
            j_hot = jnp.where(j_iota == j_at, 1.0, 0.0).astype(BF16)
            mask = dot(k_hot.astype(BF16), j_hot, NT)
            picked = dot(coef.astype(BF16), j_hot)
            rows.append(jnp.sum(picked * k_hot, axis=0, keepdims=True))
            masked.append(coef * mask)
        fields = two_sided(masked, *inverse)
        for i, row, old, field in zip(tiles, rows, fresh, fields):
            store(i, (old - field).astype(BF16), row)
        return carry

    lax.fori_loop(0, count // unroll, body, 0)


def tile_at(start):
    return pl.ds(pl.multiple_of(start, TILE), TILE)


def encode_own(momentum_ref, grad_ref, index_ref, *refs):
    table_refs, (out_ref, kept_ref) = refs[:6], refs[6:]
    columns = grad_ref.shape[1]
    count = columns // TILE
    first = lax.axis_index("section") * count

    def store(i, value, row):
        out_ref[:, tile_at(i * TILE)] = value
        kept_ref[pl.ds(i, 1), :] = row

    encode_tiles(
        count, first, lambda i: momentum_ref[:, tile_at((first + i) * TILE)],
        lambda i: grad_ref[:, tile_at(i * TILE)], index_ref, table_refs, store,
    )


def encode_rest(sections, momentum_ref, own_ref, own_kept_ref, index_ref, *refs):
    grad_refs, refs = refs[: sections - 1], refs[sections - 1 :]
    table_refs, (out_ref, rounded_ref, kept_ref) = refs[:6], refs[6:]
    columns = own_ref.shape[1]
    count = columns // TILE
    me = lax.axis_index("section")

    def copy(i, carry):
        out_ref[:, tile_at((me * count + i) * TILE)] = own_ref[:, tile_at(i * TILE)]
        kept_ref[pl.ds(me * count + i, 1), :] = own_kept_ref[pl.ds(i, 1), :]
        return carry

    lax.fori_loop(0, count, copy, 0)
    for step, grad_ref in enumerate(grad_refs, 1):
        first = lax.rem(me + sections - step, sections) * count

        def store(i, value, row, first=first):
            out_ref[:, tile_at((first + i) * TILE)] = value
            kept_ref[pl.ds(first + i, 1), :] = row

        encode_tiles(
            count, first, lambda i: momentum_ref[:, tile_at((first + i) * TILE)],
            lambda i: grad_ref[:, tile_at(i * TILE)], index_ref, table_refs, store,
        )
    rounded_ref[...] = kept_ref[...].astype(BF16)


def decode_kernel(kept_ref, index_ref, il, irh, irl, out_ref):
    columns = out_ref.shape[1]
    per = TILE // BLOCK
    replicas, _, lanes = index_ref.shape
    entries = replicas // per * lanes
    inverse = (il[...], irh[...], irl[...])
    iota = lax.broadcasted_iota(jnp.int32, (BLOCK, entries), 0).astype(F32).astype(BF16)
    zero, one = jnp.zeros((), BF16), jnp.ones((), BF16)
    slot = lax.broadcasted_iota(jnp.int32, (1, lanes), 1) // (lanes // per)
    unroll = math.gcd(4, columns // TILE)

    def merged(rows, b):
        parts = []
        for q in range(0, replicas, per):
            part = rows[q]
            for p in range(1, per):
                part = jnp.where(slot == (b + p) % per, rows[q + p], part)
            parts.append(part)
        return jnp.concatenate(parts, axis=1)

    def body(n, carry):
        sums = []
        for u in range(unroll):
            i = n * unroll + u
            values = [kept_ref[q, pl.ds(i, 1), :] for q in range(replicas)]
            indices = [index_ref[q, pl.ds(i, 1), :] for q in range(replicas)]
            blocks = []
            for b in range(per):
                index = merged(indices, b)
                k_row = (index >> 6).astype(F32).astype(BF16)
                j_row = (index & 63).astype(F32).astype(BF16)
                k_hot = jnp.where(iota == k_row, merged(values, b).astype(BF16), zero)
                j_hot = jnp.where(iota == j_row, one, zero)
                blocks.append(dot(k_hot, j_hot, NT))
            sums.append(jnp.concatenate(blocks, axis=1))
        for u, field in enumerate(two_sided(sums, *inverse)):
            out_ref[:, tile_at((n * unroll + u) * TILE)] = field.astype(BF16)
        return carry

    lax.fori_loop(0, columns // TILE // unroll, body, 0)


MESH = pl.DeviceIdType.MESH


def inner_of(count):
    return math.gcd(4, count)


def neighbours(count):
    inner = inner_of(count)
    me = lax.axis_index("dp")
    place = lax.rem(me, inner)
    base = me - place
    near = [base + lax.rem(place + k, inner) for k in range(1, inner)]
    far = [lax.rem(me + k * inner, count) for k in range(1, count // inner)]
    return me, base, near, far


def gather_near(value_ref, out_ref, send_sem, recv_sem):
    me, _, near, _ = neighbours(out_ref.shape[0])
    section = lax.axis_index("section")
    copies = []
    for k, peer in enumerate(near):
        copies.append(
            pltpu.make_async_remote_copy(
                src_ref=value_ref, dst_ref=out_ref.at[me],
                send_sem=send_sem.at[k], recv_sem=recv_sem.at[k],
                device_id=(section, peer), device_id_type=MESH,
            )
        )
        copies[-1].start()
    return copies


def gather_far(out_ref, send_sem, recv_sem):
    _, base, near, far = neighbours(out_ref.shape[0])
    section = lax.axis_index("section")
    group = out_ref.at[pl.ds(base, len(near) + 1)]
    copies = []
    for k, peer in enumerate(far):
        copies.append(
            pltpu.make_async_remote_copy(
                src_ref=group, dst_ref=group,
                send_sem=send_sem.at[len(near) + k], recv_sem=recv_sem.at[len(near) + k],
                device_id=(section, peer), device_id_type=MESH,
            )
        )
        copies[-1].start()
    return copies


def gather_count(count):
    inner = inner_of(count)
    return inner - 1 + count // inner - 1


def gather_kernel(value_ref, out_ref, held_ref, own_sem, send_sem, recv_sem):
    count = out_ref.shape[0]
    me, section = lax.axis_index("dp"), lax.axis_index("section")
    peers = [lax.rem(me + k, count) for k in range(1, count)]
    barrier = pltpu.get_barrier_semaphore()
    for peer in peers:
        pl.semaphore_signal(barrier, inc=1, device_id=(section, peer), device_id_type=MESH)
    own = pltpu.make_async_copy(value_ref, held_ref.at[me], own_sem)
    own.start()
    pl.semaphore_wait(barrier, count - 1)
    copies = []
    for k, peer in enumerate(peers):
        copies.append(
            pltpu.make_async_remote_copy(
                src_ref=value_ref, dst_ref=held_ref.at[me],
                send_sem=send_sem.at[k], recv_sem=recv_sem.at[k],
                device_id=(section, peer), device_id_type=MESH,
            )
        )
        copies[-1].start()
    own.wait()
    for copy in copies:
        copy.wait()
    out_ref[...] = held_ref[...].astype(F32)


def gather(value, collective_id):
    count = lax.axis_size("dp")
    dma = pltpu.SemaphoreType.DMA
    shape = (count,) + value.shape
    return pl.pallas_call(
        gather_kernel,
        out_shape=jax.ShapeDtypeStruct(shape, F32),
        in_specs=[VMEM],
        out_specs=VMEM,
        scratch_shapes=[pltpu.VMEM(shape, value.dtype), dma] + [dma((count - 1,))] * 2,
        compiler_params=pltpu.CompilerParams(collective_id=collective_id, has_side_effects=True),
    )(value)


CHUNKS = 4


def window_kernel(sections, weight_ref, index_ref, out_ref, index_out, local_sem, own_sem, send_sem, recv_sem,
                  pass_send, pass_recv, index_send, index_recv):
    half = out_ref.shape[2] // 2
    columns = 2 * half
    piece = out_ref.shape[1] // CHUNKS
    me, _, near, far = neighbours(index_out.shape[0])
    section = lax.axis_index("section")
    twin = me + 1 - 2 * lax.rem(me, 2)
    mine = lax.rem(me, 2)
    others = [lax.rem(section + k, sections) for k in range(1, sections)]
    barrier = pltpu.get_barrier_semaphore()
    for other in others:
        pl.semaphore_signal(barrier, inc=1, device_id=(other, me), device_id_type=MESH)
    for peer in near + far:
        pl.semaphore_signal(barrier, inc=1, device_id=(section, peer), device_id_type=MESH)
    own = pltpu.make_async_copy(
        weight_ref.at[:, pl.ds(pl.multiple_of(section * columns, columns), columns)],
        out_ref.at[section], local_sem,
    )
    own.start()
    own_index = pltpu.make_async_copy(index_ref, index_out.at[me], own_sem)
    own_index.start()
    pl.semaphore_wait(barrier, len(others) + len(near) + len(far))
    my_half = pl.ds(pl.multiple_of(mine * half, half), half)
    sends = []
    for c in range(CHUNKS):
        lines = pl.ds(c * piece, piece)
        for k, other in enumerate(others):
            source = pl.ds(pl.multiple_of(other * columns + mine * half, half), half)
            sends.append(
                pltpu.make_async_remote_copy(
                    src_ref=weight_ref.at[lines, source], dst_ref=out_ref.at[section, lines, my_half],
                    send_sem=send_sem.at[len(sends)], recv_sem=recv_sem.at[len(sends)],
                    device_id=(other, me), device_id_type=MESH,
                )
            )
            sends[-1].start()
    index_copies = gather_near(index_ref, index_out, index_send, index_recv)
    own_index.wait()
    for copy in index_copies:
        copy.wait()
    waiting = gather_far(index_out, index_send, index_recv)
    for n, send in enumerate(sends):
        send.wait_recv()
        layer = lax.rem(section + sections - 1 - n % (sections - 1), sections)
        lines = pl.ds(n // (sections - 1) * piece, piece)
        half_ref = out_ref.at[layer, lines, my_half]
        waiting.append(
            pltpu.make_async_remote_copy(
                src_ref=half_ref, dst_ref=half_ref,
                send_sem=pass_send.at[n], recv_sem=pass_recv.at[n],
                device_id=(section, twin), device_id_type=MESH,
            )
        )
        waiting[-1].start()
    for copy in waiting:
        copy.wait()
    for send in sends:
        send.wait_send()
    own.wait()


def windows(weight, index, sections, collective_id):
    count = lax.axis_size("dp")
    dma = pltpu.SemaphoreType.DMA
    rows, width = weight.shape
    return pl.pallas_call(
        functools.partial(window_kernel, sections),
        out_shape=(
            jax.ShapeDtypeStruct((sections, rows, width // sections), weight.dtype),
            jax.ShapeDtypeStruct((count,) + index.shape, index.dtype),
        ),
        in_specs=[VMEM, VMEM],
        out_specs=(VMEM, VMEM),
        scratch_shapes=[dma] * 2 + [dma(((sections - 1) * CHUNKS,))] * 4 + [dma((gather_count(count),))] * 2,
        compiler_params=pltpu.CompilerParams(collective_id=collective_id, has_side_effects=True),
    )(weight, index)


def call(kernel, out_shape, *args, scratch=()):
    return pl.pallas_call(
        kernel,
        out_shape=out_shape,
        in_specs=[VMEM] * len(args),
        out_specs=jax.tree.map(lambda _: VMEM, out_shape),
        scratch_shapes=scratch,
        cost_estimate=pl.CostEstimate(flops=10**9, bytes_accessed=4 * 2**20, transcendentals=0),
    )(*args)


def shifts(axis):
    count = lax.axis_size(axis)
    for step in range(1, count):
        yield step, [(source, (source + step) % count) for source in range(count)]


def local(inputs, cotangent, weights, momentum, keep_index):
    sections = lax.axis_size("section")
    replicas = lax.axis_size("dp")
    me = lax.axis_index("section")
    rows, width = weights.shape[1:]
    columns = inputs.shape[1]
    groups, kept_count = keep_index.shape[2:]
    per = TILE // BLOCK
    tiles = groups // per
    index = keep_index[0, 0].reshape(tiles, per * kept_count)
    index = jnp.roll(index, lax.axis_index("dp") % per * kept_count, axis=1)

    window, index_all = windows(weights[0], index, sections, 0)
    window = window.reshape(sections * rows, columns)
    stack = jnp.concatenate([inputs, cotangent, window], axis=0)
    sums = lax.dot_general(stack, window, NT, preferred_element_type=F32)
    rounded = sums.astype(BF16)
    got = [lax.ppermute(rounded, "section", pairs) for _, pairs in shifts("section")]
    got = functools.reduce(jnp.add, [part.astype(F32) for part in got]) if len(got) > 1 else got[0]
    depth = 2 * (inputs.shape[0] + sections * rows)
    grads = call(
        functools.partial(grads_kernel, sections),
        [jax.ShapeDtypeStruct((rows, columns), BF16)] * sections,
        sums, got, inputs, cotangent, window,
        scratch=[pltpu.VMEM((sections, rows, depth), BF16)],
    )
    received = [
        lax.ppermute(grads[step], "section", pairs) for step, pairs in shifts("section")
    ]
    inverse = tables(True)
    every = tables(False) + inverse
    own_tiles = columns // TILE
    own_out, own_kept = call(
        encode_own,
        (
            jax.ShapeDtypeStruct((rows, columns), BF16),
            jax.ShapeDtypeStruct((own_tiles, per * kept_count), F32),
        ),
        momentum[0, 0], grads[0], index, *every,
    )
    momentum_out, kept = call(
        functools.partial(encode_rest, sections),
        (
            jax.ShapeDtypeStruct((rows, width), BF16),
            jax.ShapeDtypeStruct((tiles, per * kept_count), BF16),
        ),
        momentum[0, 0], own_out, own_kept, index, *received, *every,
        scratch=[pltpu.VMEM((tiles, per * kept_count), F32)],
    )
    kept_all = gather(kept, 1)
    update = call(
        decode_kernel,
        jax.ShapeDtypeStruct((rows, width), BF16),
        kept_all, index_all, *inverse,
    )
    return momentum_out[None, None], update[None, None]


def solution(mesh):
    return jax.shard_map(
        local,
        mesh=mesh,
        in_specs=(
            P("dp", "section"),
            P("dp", "section"),
            P("section", None, None),
            P("section", "dp", None, None),
            P("section", "dp", None, None),
        ),
        out_specs=(P("section", "dp", None, None), P("section", "dp", None, None)),
        check_vma=False,
    )
```
